32 devices in a mesh: cuts: 4 (over y, x), space: 8 (over z, core).
Axes of the slice: x: 2, y: 2, z: 4, core: 2. Of those that a mesh axis runs over, the one named last changes fastest.
Arguments:
- starts: float32 [4, 3, 32, 64, 128], P('cuts', None, 'space'), may hold values from -3 to 3
Outputs:
- new_starts: float32 [4, 3, 32, 64, 128], P('cuts', None, 'space')
The draws below stay inside these ranges and needn't reach their ends.
All inputs are finite; a program needn't handle non-finite values.
Results may differ from the reference program's by a relative error of at most 0.0001.
Values sent between devices are 32-bit elements; how exact they have to be, the bound alone decides.
A program may use at most 64 MiB of HBM per device.

```python
import jax
import jax.numpy as jnp
from jax import lax

NY = 64
NZ = 128
FSTEPS = 16
CSTEPS = 2
SLICES = 4
NX = 32


def steps_of(stream_key, shape, cuts, least, largest):
    loudness, own = 1.0, jax.random.fold_in(stream_key, 6)
    for axis_at, shards_of in cuts:
        draws = jnp.exp(jax.random.uniform(jax.random.fold_in(own, axis_at), (shards_of,), jnp.float32, least / len(cuts), largest / len(cuts)))
        loudness = loudness * jnp.repeat(draws, shape[axis_at] // shards_of).reshape([-1 if axis == axis_at else 1 for axis in range(len(shape))])
    return loudness


def gaussian(key, extent, scale, bound, cuts=(), kind=jnp.bfloat16):
    gain = steps_of(key, extent, cuts, -0.22, 0.18) if cuts else 1.0
    result = jax.random.normal(key, extent, jnp.float32) * scale * gain
    return jnp.minimum(jnp.maximum(result, -bound), bound).astype(kind)


def setup_inputs(seed: int = 0) -> dict:
    key_of = jax.random.split(jax.random.key(seed), 2)
    starts = gaussian(key_of[0], (SLICES, 3, NX, NY, NZ), 0.5, 3.0, ((0, 4), (2, 8)), jnp.float32)
    return {"starts": starts}


fine_rate = 0.08
fine_advect = 0.04
coarse_rate = 0.16
coarse_advect = 0.16


def advance(extended, rate, advect):
    padded = jnp.pad(extended, ((0, 0), (0, 0), (1, 1), (1, 1)))
    centre = padded[:, 1:-1, 1:-1, 1:-1]
    x_plus = padded[:, 2:, 1:-1, 1:-1]
    x_minus = padded[:, :-2, 1:-1, 1:-1]
    y_plus = padded[:, 1:-1, 2:, 1:-1]
    y_minus = padded[:, 1:-1, :-2, 1:-1]
    z_plus = padded[:, 1:-1, 1:-1, 2:]
    z_minus = padded[:, 1:-1, 1:-1, :-2]
    laplace = (x_plus + x_minus) + (y_plus + y_minus) + (z_plus + z_minus) - 6.0 * centre
    convect = centre[0:1] * (x_plus - x_minus) + centre[1:2] * (y_plus - y_minus) + centre[2:3] * (z_plus - z_minus)
    return centre + rate * laplace - advect * convect


def one_step(field, rate, advect):
    return advance(jnp.pad(field, ((0, 0), (1, 1), (0, 0), (0, 0))), rate, advect)


def fine_whole(field):
    return lax.fori_loop(0, FSTEPS, lambda index, state: one_step(state, fine_rate, fine_advect), field)


def coarse_whole(field):
    return lax.fori_loop(0, CSTEPS, lambda index, state: one_step(state, coarse_rate, coarse_advect), field)


def restrict(field):
    blocks = field.reshape(field.shape[0], field.shape[1] // 2, 2, field.shape[2] // 2, 2, field.shape[3] // 2, 2)
    return jnp.sum(blocks, axis=(2, 4, 6)) * 0.125


def prolong(field):
    return jnp.repeat(jnp.repeat(jnp.repeat(field, 2, axis=1), 2, axis=2), 2, axis=3)


def reference(starts):
    ends = lax.map(fine_whole, starts)
    old_coarse = lax.map(lambda field: coarse_whole(restrict(field)), starts)
    change = ends - lax.map(prolong, old_coarse)

    def sweep(state, previous):
        advanced = coarse_whole(state)
        corrected = prolong(advanced) + previous
        return advanced + restrict(previous), corrected

    unused, corrected = lax.scan(sweep, restrict(starts[0]), change[:-1])
    return jnp.concatenate([starts[:1], corrected], axis=0)
```

```python
import functools

import jax
import jax.numpy as jnp
from jax import lax
from jax.experimental import pallas as pl
from jax.experimental.pallas import tpu as pltpu
from jax.sharding import PartitionSpec as P

FSTEPS = 16
CSTEPS = 2

fine_rate = 0.08
fine_advect = 0.04
coarse_rate = 0.16
coarse_advect = 0.16

PAD = 8
MESH = pl.DeviceIdType.MESH


def step(src, dst, items, rows, rate, advect, shift, turn):
    lanes = src.shape[-1]
    lane = lax.broadcasted_iota(jnp.int32, (8, lanes), 1)
    first, last = lane < shift, lane >= lanes - shift
    rzp, azp = jnp.where(last, 0.0, rate), jnp.where(last, 0.0, advect)
    rzm, azm = jnp.where(first, 0.0, rate), jnp.where(first, 0.0, advect)
    for row in range(rows[0], rows[1], 8):
        for si, di, keep in items:
            v = [src[si, c, pl.ds(row, 8), :] for c in range(3)]
            ax, ay = (advect * turn) * v[0], advect * v[1]
            xp, xm, yp, ym = rate - ax, rate + ax, rate - ay, rate + ay
            zp, zm = rzp - azp * v[2], rzm + azm * v[2]
            for c in range(3):
                x_part = xp * src[si + 1, c, pl.ds(row, 8), :] + xm * src[si - 1, c, pl.ds(row, 8), :]
                y_part = yp * src[si, c, pl.ds(row + 1, 8), :] + ym * src[si, c, pl.ds(row - 1, 8), :]
                z_part = zp * pltpu.roll(v[c], lanes - shift, 1) + zm * pltpu.roll(v[c], shift, 1)
                value = ((1.0 - 6.0 * rate) * v[c] + x_part) + (y_part + z_part)
                dst[di, c, pl.ds(row, 8), :] = value if keep is None else value * keep


def kernel(S, N, x_ref, out_ref, ev, od, ca, cb, cc, pk_old, pk_r, pk_cs, pk_adv, rc_old, rc_own, rc_z, rc_r, rc_rz, rc_r1,
           rc_adv, rc_end, spread, load_sem, halo_s, halo_r, part_s, part_r, mid_s, mid_r, end_s, end_r, old_s, old_r,
           own_s, own_r, z_s, z_r, r_s, r_r, rz_s, rz_r, r1_s, r1_r,
           adv_s, adv_r):
    n, s = lax.axis_index("cuts"), lax.axis_index("space")
    W, NY, NZ = x_ref.shape[2], x_ref.shape[3], x_ref.shape[4]
    CW, CY, Q, D = W // 2, NY // 2, 4 * W, 2 * W
    ROUNDS = FSTEPS // D
    END = FSTEPS // 2
    p = lax.rem(s, 2)
    way = 1 - 2 * p
    turn = way.astype(jnp.float32)
    near, mate = s - way, s + way
    far, beyond = s - 2 * way, s + 2 * way
    wall = (near < 0) | (near >= S)
    mate_wall = (beyond < 0) | (beyond >= S)
    inside = jnp.logical_not(wall)
    mate_inside = jnp.logical_not(mate_wall)
    works = n < N - 1

    def wrap(i):
        return lax.rem(i + 2 * S, S)

    def column(i):
        return lax.rem(i, N)

    pairs = [(n, near, inside), (n, mate, n >= 0)]
    pairs += [(n, far, inside & (n >= 3)), (n, beyond, mate_inside & (n >= 3))]
    pairs += [(n + 1, s, n < N - 1), (n - 1, s, n > 0)]
    pairs += [(n + 2, s, (n > 0) & (n < N - 2)), (n - 2, s, n > 2)]
    pairs += [(n + 3, s, n == 0), (n - 3, s, n == 3)]
    barrier = pltpu.get_barrier_semaphore()
    count = 0
    for i, j, cond in pairs:
        @pl.when(cond)
        def _():
            pl.semaphore_signal(barrier, inc=1, device_id=(i, j), device_id_type=MESH)
        count = count + jnp.where(cond, 1, 0)

    inner = pl.ds(PAD, NY)

    def load(i):
        return pltpu.make_async_copy(x_ref.at[0, :, i + p * (W - 1 - 2 * i)], ev.at[D + i, :, inner], load_sem.at[i])

    keep_start = pltpu.make_async_copy(x_ref.at[0], out_ref.at[0], load_sem.at[W])

    @pl.when(works)
    def _():
        for i in range(W):
            load(i).start()

    @pl.when(n == 0)
    def _():
        keep_start.start()

    zero = jnp.zeros((PAD, NZ), jnp.float32)

    def clear(i, _):
        for c in range(3):
            for top in (0, PAD + NY):
                ev[i, c, pl.ds(top, PAD), :] = zero
                od[i, c, pl.ds(top, PAD), :] = zero
        return 0

    def clear_layer(i, _):
        for c in range(3):
            for row in range(PAD, PAD + NY, 8):
                ev[i * Q + D - 1, c, pl.ds(row, 8), :] = zero
                od[i * Q + D - 1, c, pl.ds(row, 8), :] = zero
        return 0

    def clear_start(i, _):
        for c in range(3):
            for row in range(PAD, PAD + NY, 8):
                ev[i, c, pl.ds(row, 8), :] = zero
        return 0

    def clear_coarse(i, _):
        for c in range(3):
            for top in (0, PAD + CY):
                ca[i, c, pl.ds(top, PAD), :] = zero
                cb[i, c, pl.ds(top, PAD), :] = zero
        return 0

    lax.fori_loop(0, END * Q, clear, 0)
    lax.fori_loop(0, jnp.where(wall, END, 0), clear_layer, 0)
    lax.fori_loop(0, jnp.where(wall, D, 0), clear_start, 0)
    lax.fori_loop(0, 5 * CW, clear_coarse, 0)

    @pl.when(works)
    def _():
        for i in range(W):
            load(i).wait()

    pl.semaphore_wait(barrier, count)

    def remote(src, dst, send_sem, recv_sem, target):
        return pltpu.make_async_remote_copy(
            src_ref=src, dst_ref=dst, send_sem=send_sem, recv_sem=recv_sem, device_id=target, device_id_type=MESH)

    def halo(r, d):
        at = r * W * Q
        return remote(ev.at[at + D + d, :, inner], ev.at[at + D - 1 - d, :, inner], halo_s.at[r, d], halo_r.at[r, d],
                      (n, wrap(near)))

    def to_mate(r, i):
        at = r * W * Q
        return remote(ev.at[at + D + i, :, inner], ev.at[at + Q - 1 - i, :, inner], part_s.at[r, i], part_r.at[r, i],
                      (n, wrap(mate)))

    def mid_to_mate(r, i):
        at = (r * W + CW) * Q
        return remote(ev.at[at + D + i, :, inner], ev.at[at + Q - 1 - i, :, inner], mid_s.at[r, i], mid_r.at[r, i],
                      (n, wrap(mate)))

    def send_halo(r, d):
        @pl.when(inside)
        def _():
            halo(r, d).start()

    def to_next(i):
        return remote(ev.at[END * Q + D + i, :, inner], rc_end.at[i], end_s.at[i], end_r.at[i], (column(n + 1), s))

    even = lax.broadcasted_iota(jnp.int32, (CY, NZ), 1) % 2 == 0
    crow = pl.ds(PAD, CY)

    def restricted(at, c):
        def read(l, r):
            return ev[at + l, c, pl.ds(PAD + r, CY, stride=2), :]
        total = (read(0, 0) + read(0, 1)) + (read(1, 0) + read(1, 1))
        other = jnp.where(even, pltpu.roll(total, NZ - 1, 1), pltpu.roll(total, 1, 1))
        return (total + other) * 0.125

    def packed(a, b):
        return jnp.where(even, a, b)

    def unpacked(v):
        return jnp.where(even, v, pltpu.roll(v, 1, 1)), jnp.where(even, pltpu.roll(v, NZ - 1, 1), v)

    near_keep = jnp.where(wall, jnp.zeros((8, NZ), jnp.float32), 1.0)
    beyond_keep = jnp.where(mate_wall, jnp.zeros((8, NZ), jnp.float32), 1.0)

    def coarse(src, dst, lo, hi):
        items = [(c, c, near_keep if c < 2 * CW else beyond_keep if c >= 4 * CW else None) for c in range(lo, hi)]
        step(src, dst, items, (PAD, PAD + CY), coarse_rate, coarse_advect, 2, turn)

    def fine(at, l, qs):
        e, o = ev.at[pl.ds(at, W * Q + 2 * D)], od.at[pl.ds(at, (W - 1) * Q + 2 * D)]
        src, dst = (e, o) if l % 2 else (o, e)
        step(src, dst, [((l - 1) // 2 * Q + q, l // 2 * Q + q, None) for q in qs], (PAD, PAD + NY), fine_rate, fine_advect, 1, turn)

    send_old = remote(pk_old, rc_old, old_s, old_r, (column(n + 1), s))

    def one_round(r, _):
        base = r * W
        for m in range(W):
            i = W - 1 - m
            if m == 0:
                @pl.when(r == 0)
                def _():
                    to_mate(r, i).wait_recv()
                    send_halo(r, W)
            else:
                to_mate(r, i).wait_recv()
                send_halo(r, W + m)
        for l in range(1, W):
            def pair(h, _):
                fine(base * Q + 2 * h, l, [D + l, D + l + 1])
                return 0
            lax.fori_loop(0, W - l, pair, 0)

        @pl.when(r == ROUNDS - 1)
        def _():
            def restrict_layer(c, _):
                for k in range(3):
                    ca[c, k, crow, :] = restricted(2 * c, k)
                return 0
            lax.fori_loop(CW, 4 * CW, restrict_layer, 0)
            coarse(ca, cb, 2 * CW - 1, 3 * CW + 1)
            coarse(cb, cc, 2 * CW, 3 * CW)
            for k in range(3):
                pk_old[k] = packed(cc[2 * CW, k, crow, :], cc[2 * CW + 1, k, crow, :])
            send_old.start()

        def wave(k, levels):
            at = base * Q + D - 1 - k

            @pl.when(inside)
            def _():
                for l in levels:
                    fine(at, l, [l])

            @pl.when(wall)
            def _():
                for l in levels:
                    @pl.when(l > k)
                    def _():
                        fine(at, l, [l])

        def await_halo(k):
            @pl.when(inside)
            def _():
                halo(r, k).wait_recv()

        def early(k, _):
            await_halo(k)
            wave(k, range(1, W + 1))

            @pl.when(k < W)
            def _():
                mid_to_mate(r, W - 1 - k).start()

            @pl.when(k >= 1)
            def _():
                mid_to_mate(r, W - k).wait_recv()

            @pl.when(k >= 2)
            def _():
                for l in range(W + 1, D):
                    fine(base * Q + k, l, [Q - 1 - l])

            @pl.when(k >= 1)
            def _():
                wave(k, range(W + 1, D))
            return 0

        lax.fori_loop(0, W + 1, early, 0)
        wave(W, [D])

        def sent(k):
            i = D - 1 - k

            @pl.when(r < ROUNDS - 1)
            def _():
                to_mate(r + 1, i).start()
                if k == W:
                    send_halo(r + 1, i)
                elif k == W + 1:
                    send_halo(r + 1, i)
                    to_mate(r + 1, W - 1).wait_recv()
                    send_halo(r + 1, W)
                elif k == D - 1:
                    send_halo(r + 1, 0)
                    send_halo(r + 1, 1)

            @pl.when(r == ROUNDS - 1)
            def _():
                if k == W:
                    to_next(i).start()

        sent(W)

        def late(k, _):
            await_halo(k)
            wave(k, range(1, D + 1))
            for j in range(W + 1, D):
                @pl.when(k == j)
                def _():
                    sent(j)
            return 0

        lax.fori_loop(W + 1, D, late, 0)
        return 0

    def own_copy(target):
        return remote(pk_cs, rc_own, own_s, own_r, (column(target), s))

    adv_copy = remote(pk_adv, rc_adv, adv_s, adv_r, (column(n + N - 1), s))

    def r_copy(target):
        return remote(pk_r, rc_r, r_s, r_r, (column(target), s))

    def r1_copy(target):
        return remote(pk_r, rc_r1, r1_s, r1_r, (column(target), s))

    @pl.when(works)
    def _():
        for i in range(W):
            send_halo(0, i)
            to_mate(0, W - 1 - i).start()
        lax.fori_loop(0, ROUNDS, one_round, 0)
        for k in range(3):
            change = [restricted(END * Q + D + 2 * j, k) - cc[2 * CW + j, k, crow, :] for j in range(CW)]
            pk_r[k] = packed(*change)
            pk_cs[k] = packed(*(cc[2 * CW + j, k, crow, :] + change[j] for j in range(CW)))

        @pl.when(n == 0)
        def _():
            own_copy(3).start()

        @pl.when((n >= 1) & (n <= N - 3))
        def _():
            r_copy(n + 2).start()
        if N > 4:
            @pl.when((n >= 1) & (n <= N - 4))
            def _():
                r1_copy(n + 1).start()
        for i in range(W - 2, -1, -1):
            to_next(i).start()

    def exchange(src, dst, send, recv, k):
        target, slot = [(near, 0), (mate, 1), (far, 3), (beyond, 2)][k]
        return remote(src, dst.at[slot], send.at[slot], recv.at[slot], (n, wrap(target)))

    exists = [inside, None, inside, mate_inside]

    def guarded(cond, do):
        if cond is None:
            do()
        else:
            pl.when(cond)(do)

    places = [(2 * CW - 1, -1), (4 * CW - 1, -1), (0, 1), (4 * CW, 1)]
    slot_exists = [inside, None, inside, mate_inside]

    def unpack_into(dst, slot, src):
        first, by = places[slot]

        def fill():
            for k in range(3):
                for j, v in enumerate(unpacked(src[k])):
                    dst[first + by * j, k, crow, :] = v

        def blank():
            for k in range(3):
                for j in range(CW):
                    dst[first + by * j, k, crow, :] = jnp.zeros((CY, NZ), jnp.float32)

        guarded(slot_exists[slot], fill)
        if slot_exists[slot] is not None:
            pl.when(jnp.logical_not(slot_exists[slot]))(blank)

    @pl.when(n == 1)
    def _():
        old_copy = remote(pk_old, rc_old, old_s, old_r, (column(n + 1), s))
        old_copy.wait_recv()
        for k in range(3):
            for j, v in enumerate(unpacked(rc_old[k])):
                cc[2 * CW + j, k, crow, :] = v

    @pl.when(n == 2)
    def _():
        adv_copy.wait_recv()
        for k in range(3):
            for j, v in enumerate(unpacked(rc_adv[k])):
                cc[2 * CW + j, k, crow, :] = v

    @pl.when(n >= 3)
    def _():
        own_copy(n + 2).wait_recv()
        for k in range(4):
            guarded(exists[k], lambda: exchange(rc_own, rc_z, z_s, z_r, k).start())
        for k in range(3):
            for j, v in enumerate(unpacked(rc_own[k])):
                ca[2 * CW + j, k, crow, :] = v
        r_copy(n + 2).wait_recv()
        for k in range(2):
            guarded(exists[k], lambda: exchange(rc_r, rc_rz, rz_s, rz_r, k).start())
        for k, slot in ((1, 1), (0, 0), (2, 3), (3, 2)):
            guarded(slot_exists[slot], lambda: exchange(rc_own, rc_z, z_s, z_r, k).wait_recv())
            unpack_into(ca, slot, rc_z.at[slot])
        coarse(ca, cb, 1, 5 * CW - 1)
        coarse(cb, cc, CW, 4 * CW)

        @pl.when(n == 3)
        def _():
            for k in range(3):
                pk_adv[k] = packed(cc[2 * CW, k, crow, :], cc[2 * CW + 1, k, crow, :])
            adv_copy.start()
        for slot in (1, 0):
            guarded(slot_exists[slot], lambda: exchange(rc_r, rc_rz, rz_s, rz_r, slot).wait_recv())
            unpack_into(ca, slot, rc_rz.at[slot])
        for k in range(3):
            for j, v in enumerate(unpacked(rc_r[k])):
                ca[2 * CW + j, k, crow, :] = v

        def add(c, _):
            for k in range(3):
                ca[c, k, crow, :] = ca[c, k, crow, :] + cc[c, k, crow, :]
            return 0

        lax.fori_loop(CW, 4 * CW, add, 0)
        coarse(ca, cb, 2 * CW - 1, 3 * CW + 1)
        coarse(cb, cc, 2 * CW, 3 * CW)

    if N > 4:
        @pl.when((n >= 2) & (n <= N - 3))
        def _():
            r1_copy(n + 1).wait_recv()
            for k in range(3):
                change = unpacked(rc_r1[k])
                pk_cs[k] = packed(*(cc[2 * CW + j, k, crow, :] + change[j] for j in range(CW)))
            own_copy(n + 2).start()

    @pl.when(n == 0)
    def _():
        keep_start.wait()

    @pl.when(n > 0)
    def _():
        @pl.when(n > 1)
        def _():
            send_old.wait_recv()
        for k in range(3):
            old = unpacked(rc_old[k])
            for j in range(CW):
                rise = cc[2 * CW + j, k, crow, :] - old[j]
                for r in range(2):
                    spread[j, k, pl.ds(r, CY, stride=2), :] = rise
        for i in range(W - 1, -1, -1):
            to_next(i).wait_recv()
            for k in range(3):
                out_ref[0, k, i + p * (W - 1 - 2 * i)] = spread[i // 2, k, pl.ds(0, NY), :] + rc_end[i, k]

    @pl.when(works)
    def _():
        send_old.wait_send()
        for i in range(W):
            to_next(i).wait_send()
            for r in range(ROUNDS):
                to_mate(r, i).wait_send()
                mid_to_mate(r, i).wait_send()

        @pl.when(inside)
        def _():
            for r in range(ROUNDS):
                for d in range(D):
                    halo(r, d).wait_send()

        @pl.when(n == 0)
        def _():
            own_copy(3).wait_send()

        @pl.when((n >= 1) & (n <= N - 3))
        def _():
            r_copy(n + 2).wait_send()
        if N > 4:
            @pl.when((n >= 1) & (n <= N - 4))
            def _():
                r1_copy(n + 1).wait_send()

            @pl.when((n >= 2) & (n <= N - 3))
            def _():
                own_copy(n + 2).wait_send()

    @pl.when(n >= 3)
    def _():
        for k in range(4):
            guarded(exists[k], lambda: exchange(rc_own, rc_z, z_s, z_r, k).wait_send())
        for k in range(2):
            guarded(exists[k], lambda: exchange(rc_r, rc_rz, rz_s, rz_r, k).wait_send())

        @pl.when(n == 3)
        def _():
            adv_copy.wait_send()


def shards(S, N, starts):
    W, NY, NZ = starts.shape[2:]
    D, Q = 2 * W, 4 * W
    assert W == 4 and FSTEPS % D == 0 and CSTEPS == 2 and S % 2 == 0 and N > 3
    f32 = jnp.float32
    CW, CY, ROUNDS, END = W // 2, NY // 2, FSTEPS // D, FSTEPS // 2
    pack = (3, CY, NZ)
    coarse = pltpu.VMEM((5 * CW, 3, CY + 2 * PAD, NZ), f32)
    dma = pltpu.SemaphoreType.DMA
    return pl.pallas_call(
        functools.partial(kernel, S, N),
        out_shape=jax.ShapeDtypeStruct(starts.shape, f32),
        in_specs=[pl.BlockSpec(memory_space=pltpu.HBM)],
        out_specs=pl.BlockSpec(memory_space=pltpu.VMEM),
        scratch_shapes=[
            pltpu.VMEM(((END + 1) * Q + D, 3, NY + 2 * PAD, NZ), f32),
            pltpu.VMEM((END * Q + D, 3, NY + 2 * PAD, NZ), f32),
            coarse, coarse, coarse,
            pltpu.VMEM(pack, f32), pltpu.VMEM(pack, f32), pltpu.VMEM(pack, f32), pltpu.VMEM(pack, f32),
            pltpu.VMEM(pack, f32), pltpu.VMEM(pack, f32), pltpu.VMEM((4,) + pack, f32),
            pltpu.VMEM(pack, f32), pltpu.VMEM((2,) + pack, f32), pltpu.VMEM(pack, f32), pltpu.VMEM(pack, f32),
            pltpu.VMEM((W, 3, NY, NZ), f32),
            pltpu.VMEM((CW, 3, NY + PAD, NZ), f32),
            dma((W + 1,)),
            dma((ROUNDS, D)), dma((ROUNDS, D)), dma((ROUNDS, W)), dma((ROUNDS, W)), dma((ROUNDS, W)), dma((ROUNDS, W)),
            dma((W,)), dma((W,)), dma, dma, dma, dma, dma((4,)), dma((4,)), dma, dma, dma((2,)), dma((2,)), dma, dma, dma, dma,
        ],
        compiler_params=pltpu.CompilerParams(collective_id=0, has_side_effects=True, vmem_limit_bytes=48 * 2**20),
    )(starts)


def solution(mesh):
    placed = P("cuts", None, "space", None, None)
    return jax.shard_map(
        functools.partial(shards, mesh.shape["space"], mesh.shape["cuts"]),
        mesh=mesh, in_specs=(placed,), out_specs=placed, check_vma=False)
```

```python
import functools

import jax
import jax.numpy as jnp
from jax import lax
from jax.experimental import pallas as pl
from jax.experimental.pallas import tpu as pltpu
from jax.sharding import PartitionSpec as P

FSTEPS = 16
CSTEPS = 2

fine_rate = 0.08
fine_advect = 0.04
coarse_rate = 0.16
coarse_advect = 0.16

PAD = 8
MESH = pl.DeviceIdType.MESH


def step(src, dst, items, rows, rate, advect, shift, turn):
    lanes = src.shape[-1]
    lane = lax.broadcasted_iota(jnp.int32, (8, lanes), 1)
    first, last = lane < shift, lane >= lanes - shift
    rzp, azp = jnp.where(last, 0.0, rate), jnp.where(last, 0.0, advect)
    rzm, azm = jnp.where(first, 0.0, rate), jnp.where(first, 0.0, advect)
    for row in range(rows[0], rows[1], 8):
        for si, di, keep in items:
            v = [src[si, c, pl.ds(row, 8), :] for c in range(3)]
            ax, ay = (advect * turn) * v[0], advect * v[1]
            xp, xm, yp, ym = rate - ax, rate + ax, rate - ay, rate + ay
            zp, zm = rzp - azp * v[2], rzm + azm * v[2]
            for c in range(3):
                x_part = xp * src[si + 1, c, pl.ds(row, 8), :] + xm * src[si - 1, c, pl.ds(row, 8), :]
                y_part = yp * src[si, c, pl.ds(row + 1, 8), :] + ym * src[si, c, pl.ds(row - 1, 8), :]
                z_part = zp * pltpu.roll(v[c], lanes - shift, 1) + zm * pltpu.roll(v[c], shift, 1)
                value = ((1.0 - 6.0 * rate) * v[c] + x_part) + (y_part + z_part)
                dst[di, c, pl.ds(row, 8), :] = value if keep is None else value * keep


def kernel(S, N, x_ref, out_ref, ev, od, ca, cb, cc, pk_old, pk_r, pk_cs, pk_adv, rc_old, rc_own, rc_z, rc_r, rc_rz, rc_r1,
           rc_adv, rc_end, spread, load_sem, halo_s, halo_r, part_s, part_r, mid_s, mid_r, end_s, end_r, old_s, old_r,
           own_s, own_r, z_s, z_r, r_s, r_r, rz_s, rz_r, r1_s, r1_r,
           adv_s, adv_r):
    n, s = lax.axis_index("cuts"), lax.axis_index("space")
    W, NY, NZ = x_ref.shape[2], x_ref.shape[3], x_ref.shape[4]
    CW, CY, Q, D = W // 2, NY // 2, 4 * W, 2 * W
    ROUNDS = FSTEPS // D
    END = FSTEPS // 2
    p = lax.rem(s, 2)
    way = 1 - 2 * p
    turn = way.astype(jnp.float32)
    near, mate = s - way, s + way
    far, beyond = s - 2 * way, s + 2 * way
    wall = (near < 0) | (near >= S)
    mate_wall = (beyond < 0) | (beyond >= S)
    inside = jnp.logical_not(wall)
    mate_inside = jnp.logical_not(mate_wall)
    works = n < N - 1

    def wrap(i):
        return lax.rem(i + 2 * S, S)

    def column(i):
        return lax.rem(i, N)

    pairs = [(n, near, inside), (n, mate, n >= 0)]
    pairs += [(n, far, inside & (n >= 3)), (n, beyond, mate_inside & (n >= 3))]
    pairs += [(n + 1, s, n < N - 1), (n - 1, s, n > 0)]
    pairs += [(n + 2, s, (n > 0) & (n < N - 2)), (n - 2, s, n > 2)]
    pairs += [(n + 3, s, n == 0), (n - 3, s, n == 3)]
    barrier = pltpu.get_barrier_semaphore()
    count = 0
    for i, j, cond in pairs:
        @pl.when(cond)
        def _():
            pl.semaphore_signal(barrier, inc=1, device_id=(i, j), device_id_type=MESH)
        count = count + jnp.where(cond, 1, 0)

    inner = pl.ds(PAD, NY)

    def load(i):
        return pltpu.make_async_copy(x_ref.at[0, :, i + p * (W - 1 - 2 * i)], ev.at[D + i, :, inner], load_sem.at[i])

    keep_start = pltpu.make_async_copy(x_ref.at[0], out_ref.at[0], load_sem.at[W])

    @pl.when(works)
    def _():
        for i in range(W):
            load(i).start()

    @pl.when(n == 0)
    def _():
        keep_start.start()

    zero = jnp.zeros((PAD, NZ), jnp.float32)

    def clear(i, _):
        for c in range(3):
            for top in (0, PAD + NY):
                ev[i, c, pl.ds(top, PAD), :] = zero
                od[i, c, pl.ds(top, PAD), :] = zero
        return 0

    def clear_layer(i, _):
        for c in range(3):
            for row in range(PAD, PAD + NY, 8):
                ev[i * Q + D - 1, c, pl.ds(row, 8), :] = zero
                od[i * Q + D - 1, c, pl.ds(row, 8), :] = zero
        return 0

    def clear_start(i, _):
        for c in range(3):
            for row in range(PAD, PAD + NY, 8):
                ev[i, c, pl.ds(row, 8), :] = zero
        return 0

    def clear_coarse(i, _):
        for c in range(3):
            for top in (0, PAD + CY):
                ca[i, c, pl.ds(top, PAD), :] = zero
                cb[i, c, pl.ds(top, PAD), :] = zero
        return 0

    lax.fori_loop(0, END * Q, clear, 0)
    lax.fori_loop(0, jnp.where(wall, END, 0), clear_layer, 0)
    lax.fori_loop(0, jnp.where(wall, D, 0), clear_start, 0)
    lax.fori_loop(0, 5 * CW, clear_coarse, 0)

    @pl.when(works)
    def _():
        for i in range(W):
            load(i).wait()

    pl.semaphore_wait(barrier, count)

    def remote(src, dst, send_sem, recv_sem, target):
        return pltpu.make_async_remote_copy(
            src_ref=src, dst_ref=dst, send_sem=send_sem, recv_sem=recv_sem, device_id=target, device_id_type=MESH)

    def halo(r, d):
        at = r * W * Q
        return remote(ev.at[at + D + d, :, inner], ev.at[at + D - 1 - d, :, inner], halo_s.at[r, d], halo_r.at[r, d],
                      (n, wrap(near)))

    def to_mate(r, i):
        at = r * W * Q
        return remote(ev.at[at + D + i, :, inner], ev.at[at + Q - 1 - i, :, inner], part_s.at[r, i], part_r.at[r, i],
                      (n, wrap(mate)))

    def mid_to_mate(r, i):
        at = (r * W + CW) * Q
        return remote(ev.at[at + D + i, :, inner], ev.at[at + Q - 1 - i, :, inner], mid_s.at[r, i], mid_r.at[r, i],
                      (n, wrap(mate)))

    def send_halo(r, d):
        @pl.when(inside)
        def _():
            halo(r, d).start()

    def to_next(i):
        return remote(ev.at[END * Q + D + i, :, inner], rc_end.at[i], end_s.at[i], end_r.at[i], (column(n + 1), s))

    even = lax.broadcasted_iota(jnp.int32, (CY, NZ), 1) % 2 == 0
    crow = pl.ds(PAD, CY)

    def restricted(at, c):
        def read(l, r):
            return ev[at + l, c, pl.ds(PAD + r, CY, stride=2), :]
        total = (read(0, 0) + read(0, 1)) + (read(1, 0) + read(1, 1))
        other = jnp.where(even, pltpu.roll(total, NZ - 1, 1), pltpu.roll(total, 1, 1))
        return (total + other) * 0.125

    def packed(a, b):
        return jnp.where(even, a, b)

    def unpacked(v):
        return jnp.where(even, v, pltpu.roll(v, 1, 1)), jnp.where(even, pltpu.roll(v, NZ - 1, 1), v)

    near_keep = jnp.where(wall, jnp.zeros((8, NZ), jnp.float32), 1.0)
    beyond_keep = jnp.where(mate_wall, jnp.zeros((8, NZ), jnp.float32), 1.0)

    def coarse(src, dst, lo, hi):
        items = [(c, c, near_keep if c < 2 * CW else beyond_keep if c >= 4 * CW else None) for c in range(lo, hi)]
        step(src, dst, items, (PAD, PAD + CY), coarse_rate, coarse_advect, 2, turn)

    def fine(at, l, qs):
        e, o = ev.at[pl.ds(at, W * Q + 2 * D)], od.at[pl.ds(at, (W - 1) * Q + 2 * D)]
        src, dst = (e, o) if l % 2 else (o, e)
        step(src, dst, [((l - 1) // 2 * Q + q, l // 2 * Q + q, None) for q in qs], (PAD, PAD + NY), fine_rate, fine_advect, 1, turn)

    send_old = remote(pk_old, rc_old, old_s, old_r, (column(n + 1), s))

    def one_round(r, _):
        base = r * W
        for m in range(W):
            i = W - 1 - m
            if m == 0:
                @pl.when(r == 0)
                def _():
                    to_mate(r, i).wait_recv()
                    send_halo(r, W)
            else:
                to_mate(r, i).wait_recv()
                send_halo(r, W + m)
        for l in range(1, W):
            def pair(h, _):
                fine(base * Q + 2 * h, l, [D + l, D + l + 1])
                return 0
            lax.fori_loop(0, W - l, pair, 0)

        @pl.when(r == ROUNDS - 1)
        def _():
            def restrict_layer(c, _):
                for k in range(3):
                    ca[c, k, crow, :] = restricted(2 * c, k)
                return 0
            lax.fori_loop(CW, 4 * CW, restrict_layer, 0)
            coarse(ca, cb, 2 * CW - 1, 3 * CW + 1)
            coarse(cb, cc, 2 * CW, 3 * CW)
            for k in range(3):
                pk_old[k] = packed(cc[2 * CW, k, crow, :], cc[2 * CW + 1, k, crow, :])
            send_old.start()

        def wave(k, levels):
            fixed = isinstance(k, int)
            at, first = (base * Q, D - 1 - k) if fixed else (base * Q + D - 1 - k, 0)

            @pl.when(inside)
            def _():
                for l in levels:
                    fine(at, l, [first + l])

            @pl.when(wall)
            def _():
                for l in levels:
                    if not fixed:
                        @pl.when(l > k)
                        def _():
                            fine(at, l, [first + l])
                    elif l > k:
                        fine(at, l, [first + l])

        def await_halo(k):
            @pl.when(inside)
            def _():
                halo(r, k).wait_recv()

        for k in range(W + 1):
            await_halo(k)
            wave(k, range(1, W + 1))
            if k < W:
                mid_to_mate(r, W - 1 - k).start()
            if k >= 1:
                mid_to_mate(r, W - k).wait_recv()
                for l in range(W + 1, W + k):
                    fine(base * Q, l, [Q - 1 + k - l])
                wave(k, range(W + 1, W + 1 + k))

        def sent(k):
            i = D - 1 - k

            @pl.when(r < ROUNDS - 1)
            def _():
                to_mate(r + 1, i).start()
                if k == W:
                    send_halo(r + 1, i)
                elif k == W + 1:
                    send_halo(r + 1, i)
                    to_mate(r + 1, W - 1).wait_recv()
                    send_halo(r + 1, W)
                elif k == D - 1:
                    send_halo(r + 1, 0)
                    send_halo(r + 1, 1)

            @pl.when(r == ROUNDS - 1)
            def _():
                if k == W:
                    to_next(i).start()
                elif i > 0:
                    pl.when(n > 0)(lambda: to_next(i).start())

        sent(W)

        def late(k, _):
            await_halo(k)
            wave(k, range(1, D + 1))
            for j in range(W + 1, D):
                @pl.when(k == j)
                def _():
                    sent(j)
            return 0

        lax.fori_loop(W + 1, D, late, 0)
        return 0

    def own_copy(target):
        return remote(pk_cs, rc_own, own_s, own_r, (column(target), s))

    adv_copy = remote(pk_adv, rc_adv, adv_s, adv_r, (column(n + N - 1), s))

    def r_copy(target):
        return remote(pk_r, rc_r, r_s, r_r, (column(target), s))

    def r1_copy(target):
        return remote(pk_r, rc_r1, r1_s, r1_r, (column(target), s))

    @pl.when(works)
    def _():
        for i in range(W):
            send_halo(0, i)
            to_mate(0, W - 1 - i).start()
        lax.fori_loop(0, ROUNDS, one_round, 0)
        for k in range(3):
            change = [restricted(END * Q + D + 2 * j, k) - cc[2 * CW + j, k, crow, :] for j in range(CW)]
            pk_r[k] = packed(*change)
            pk_cs[k] = packed(*(cc[2 * CW + j, k, crow, :] + change[j] for j in range(CW)))

        @pl.when(n == 0)
        def _():
            own_copy(3).start()

        @pl.when((n >= 1) & (n <= N - 3))
        def _():
            r_copy(n + 2).start()
        if N > 4:
            @pl.when((n >= 1) & (n <= N - 4))
            def _():
                r1_copy(n + 1).start()
        for i in range(W - 2, 0, -1):
            pl.when(n == 0)(lambda: to_next(i).start())
        to_next(0).start()

    def exchange(src, dst, send, recv, k):
        target, slot = [(near, 0), (mate, 1), (far, 3), (beyond, 2)][k]
        return remote(src, dst.at[slot], send.at[slot], recv.at[slot], (n, wrap(target)))

    exists = [inside, None, inside, mate_inside]

    def guarded(cond, do):
        if cond is None:
            do()
        else:
            pl.when(cond)(do)

    places = [(2 * CW - 1, -1), (4 * CW - 1, -1), (0, 1), (4 * CW, 1)]
    slot_exists = [inside, None, inside, mate_inside]

    def unpack_into(dst, slot, src):
        first, by = places[slot]

        def fill():
            for k in range(3):
                for j, v in enumerate(unpacked(src[k])):
                    dst[first + by * j, k, crow, :] = v

        def blank():
            for k in range(3):
                for j in range(CW):
                    dst[first + by * j, k, crow, :] = jnp.zeros((CY, NZ), jnp.float32)

        guarded(slot_exists[slot], fill)
        if slot_exists[slot] is not None:
            pl.when(jnp.logical_not(slot_exists[slot]))(blank)

    @pl.when(n == 1)
    def _():
        old_copy = remote(pk_old, rc_old, old_s, old_r, (column(n + 1), s))
        old_copy.wait_recv()
        for k in range(3):
            for j, v in enumerate(unpacked(rc_old[k])):
                cc[2 * CW + j, k, crow, :] = v

    @pl.when(n == 2)
    def _():
        adv_copy.wait_recv()
        for k in range(3):
            for j, v in enumerate(unpacked(rc_adv[k])):
                cc[2 * CW + j, k, crow, :] = v

    @pl.when(n >= 3)
    def _():
        own_copy(n + 2).wait_recv()
        for k in range(4):
            guarded(exists[k], lambda: exchange(rc_own, rc_z, z_s, z_r, k).start())
        for k in range(3):
            for j, v in enumerate(unpacked(rc_own[k])):
                ca[2 * CW + j, k, crow, :] = v
        r_copy(n + 2).wait_recv()
        for k in range(2):
            guarded(exists[k], lambda: exchange(rc_r, rc_rz, rz_s, rz_r, k).start())
        def arrived(k, slot):
            guarded(slot_exists[slot], lambda: exchange(rc_own, rc_z, z_s, z_r, k).wait_recv())
            unpack_into(ca, slot, rc_z.at[slot])

        arrived(1, 1)
        arrived(0, 0)
        coarse(ca, cb, 2 * CW - 1, 3 * CW + 1)
        coarse(cb, cc, 2 * CW, 3 * CW)

        @pl.when(n == 3)
        def _():
            for k in range(3):
                pk_adv[k] = packed(cc[2 * CW, k, crow, :], cc[2 * CW + 1, k, crow, :])
            adv_copy.start()
        arrived(2, 3)
        arrived(3, 2)
        for lo, hi in ((1, 2 * CW - 1), (3 * CW + 1, 5 * CW - 1)):
            coarse(ca, cb, lo, hi)
        for lo, hi in ((CW, 2 * CW), (3 * CW, 4 * CW)):
            coarse(cb, cc, lo, hi)
        for slot in (1, 0):
            guarded(slot_exists[slot], lambda: exchange(rc_r, rc_rz, rz_s, rz_r, slot).wait_recv())
            unpack_into(ca, slot, rc_rz.at[slot])
        for k in range(3):
            for j, v in enumerate(unpacked(rc_r[k])):
                ca[2 * CW + j, k, crow, :] = v

        def add(c, _):
            for k in range(3):
                ca[c, k, crow, :] = ca[c, k, crow, :] + cc[c, k, crow, :]
            return 0

        lax.fori_loop(CW, 4 * CW, add, 0)
        coarse(ca, cb, 2 * CW - 1, 3 * CW + 1)
        coarse(cb, cc, 2 * CW, 3 * CW)

    if N > 4:
        @pl.when((n >= 2) & (n <= N - 3))
        def _():
            r1_copy(n + 1).wait_recv()
            for k in range(3):
                change = unpacked(rc_r1[k])
                pk_cs[k] = packed(*(cc[2 * CW + j, k, crow, :] + change[j] for j in range(CW)))
            own_copy(n + 2).start()

    @pl.when(n == 0)
    def _():
        keep_start.wait()

    @pl.when(n > 0)
    def _():
        @pl.when(n > 1)
        def _():
            send_old.wait_recv()
        for k in range(3):
            old = unpacked(rc_old[k])
            for j in range(CW):
                rise = cc[2 * CW + j, k, crow, :] - old[j]
                for r in range(2):
                    spread[j, k, pl.ds(r, CY, stride=2), :] = rise
        for i in range(W - 1, -1, -1):
            to_next(i).wait_recv()
            for k in range(3):
                out_ref[0, k, i + p * (W - 1 - 2 * i)] = spread[i // 2, k, pl.ds(0, NY), :] + rc_end[i, k]

    @pl.when(works)
    def _():
        send_old.wait_send()
        for i in range(W):
            to_next(i).wait_send()
            for r in range(ROUNDS):
                to_mate(r, i).wait_send()
                mid_to_mate(r, i).wait_send()

        @pl.when(inside)
        def _():
            for r in range(ROUNDS):
                for d in range(D):
                    halo(r, d).wait_send()

        @pl.when(n == 0)
        def _():
            own_copy(3).wait_send()

        @pl.when((n >= 1) & (n <= N - 3))
        def _():
            r_copy(n + 2).wait_send()
        if N > 4:
            @pl.when((n >= 1) & (n <= N - 4))
            def _():
                r1_copy(n + 1).wait_send()

            @pl.when((n >= 2) & (n <= N - 3))
            def _():
                own_copy(n + 2).wait_send()

    @pl.when(n >= 3)
    def _():
        for k in range(4):
            guarded(exists[k], lambda: exchange(rc_own, rc_z, z_s, z_r, k).wait_send())
        for k in range(2):
            guarded(exists[k], lambda: exchange(rc_r, rc_rz, rz_s, rz_r, k).wait_send())

        @pl.when(n == 3)
        def _():
            adv_copy.wait_send()


def shards(S, N, starts):
    W, NY, NZ = starts.shape[2:]
    D, Q = 2 * W, 4 * W
    assert W == 4 and FSTEPS % D == 0 and CSTEPS == 2 and S % 2 == 0 and N > 3
    f32 = jnp.float32
    CW, CY, ROUNDS, END = W // 2, NY // 2, FSTEPS // D, FSTEPS // 2
    pack = (3, CY, NZ)
    coarse = pltpu.VMEM((5 * CW, 3, CY + 2 * PAD, NZ), f32)
    dma = pltpu.SemaphoreType.DMA
    return pl.pallas_call(
        functools.partial(kernel, S, N),
        out_shape=jax.ShapeDtypeStruct(starts.shape, f32),
        in_specs=[pl.BlockSpec(memory_space=pltpu.HBM)],
        out_specs=pl.BlockSpec(memory_space=pltpu.VMEM),
        scratch_shapes=[
            pltpu.VMEM(((END + 1) * Q + D, 3, NY + 2 * PAD, NZ), f32),
            pltpu.VMEM((END * Q + D, 3, NY + 2 * PAD, NZ), f32),
            coarse, coarse, coarse,
            pltpu.VMEM(pack, f32), pltpu.VMEM(pack, f32), pltpu.VMEM(pack, f32), pltpu.VMEM(pack, f32),
            pltpu.VMEM(pack, f32), pltpu.VMEM(pack, f32), pltpu.VMEM((4,) + pack, f32),
            pltpu.VMEM(pack, f32), pltpu.VMEM((2,) + pack, f32), pltpu.VMEM(pack, f32), pltpu.VMEM(pack, f32),
            pltpu.VMEM((W, 3, NY, NZ), f32),
            pltpu.VMEM((CW, 3, NY + PAD, NZ), f32),
            dma((W + 1,)),
            dma((ROUNDS, D)), dma((ROUNDS, D)), dma((ROUNDS, W)), dma((ROUNDS, W)), dma((ROUNDS, W)), dma((ROUNDS, W)),
            dma((W,)), dma((W,)), dma, dma, dma, dma, dma((4,)), dma((4,)), dma, dma, dma((2,)), dma((2,)), dma, dma, dma, dma,
        ],
        compiler_params=pltpu.CompilerParams(collective_id=0, has_side_effects=True, vmem_limit_bytes=48 * 2**20),
    )(starts)


def solution(mesh):
    placed = P("cuts", None, "space", None, None)
    return jax.shard_map(
        functools.partial(shards, mesh.shape["space"], mesh.shape["cuts"]),
        mesh=mesh, in_specs=(placed,), out_specs=placed, check_vma=False)
```

```python
import functools

import jax
import jax.numpy as jnp
from jax import lax
from jax.experimental import pallas as pl
from jax.experimental.pallas import tpu as pltpu
from jax.sharding import PartitionSpec as P

FSTEPS = 16
CSTEPS = 2

fine_rate = 0.08
fine_advect = 0.04
coarse_rate = 0.16
coarse_advect = 0.16

PAD = 8
MESH = pl.DeviceIdType.MESH


def step(src, dst, items, rows, rate, advect, shift, turn):
    lanes = src.shape[-1]
    lane = lax.broadcasted_iota(jnp.int32, (8, lanes), 1)
    first, last = lane < shift, lane >= lanes - shift
    rzp, azp = jnp.where(last, 0.0, rate), jnp.where(last, 0.0, advect)
    rzm, azm = jnp.where(first, 0.0, rate), jnp.where(first, 0.0, advect)
    for row in range(rows[0], rows[1], 8):
        for si, di, keep in items:
            v = [src[si, c, pl.ds(row, 8), :] for c in range(3)]
            ax, ay = (advect * turn) * v[0], advect * v[1]
            xp, xm, yp, ym = rate - ax, rate + ax, rate - ay, rate + ay
            zp, zm = rzp - azp * v[2], rzm + azm * v[2]
            for c in range(3):
                x_part = xp * src[si + 1, c, pl.ds(row, 8), :] + xm * src[si - 1, c, pl.ds(row, 8), :]
                y_part = yp * src[si, c, pl.ds(row + 1, 8), :] + ym * src[si, c, pl.ds(row - 1, 8), :]
                z_part = zp * pltpu.roll(v[c], lanes - shift, 1) + zm * pltpu.roll(v[c], shift, 1)
                value = ((1.0 - 6.0 * rate) * v[c] + x_part) + (y_part + z_part)
                dst[di, c, pl.ds(row, 8), :] = value if keep is None else value * keep


def kernel(S, N, x_ref, out_ref, ev, od, ca, cb, cc, pk_old, pk_r, pk_cs, pk_adv, rc_old, rc_own, rc_z, rc_r, rc_rz, rc_r1,
           rc_adv, rc_end, spread, load_sem, halo_s, halo_r, part_s, part_r, mid_s, mid_r, end_s, end_r, old_s, old_r,
           own_s, own_r, z_s, z_r, r_s, r_r, rz_s, rz_r, r1_s, r1_r,
           adv_s, adv_r):
    n, s = lax.axis_index("cuts"), lax.axis_index("space")
    W, NY, NZ = x_ref.shape[2], x_ref.shape[3], x_ref.shape[4]
    CW, CY, Q, D = W // 2, NY // 2, 4 * W, 2 * W
    ROUNDS = FSTEPS // D
    END = FSTEPS // 2
    p = lax.rem(s, 2)
    way = 1 - 2 * p
    turn = way.astype(jnp.float32)
    near, mate = s - way, s + way
    far, beyond = s - 2 * way, s + 2 * way
    wall = (near < 0) | (near >= S)
    mate_wall = (beyond < 0) | (beyond >= S)
    inside = jnp.logical_not(wall)
    mate_inside = jnp.logical_not(mate_wall)
    works = n < N - 1

    def wrap(i):
        return lax.rem(i + 2 * S, S)

    def column(i):
        return lax.rem(i, N)

    pairs = [(n, near, inside), (n, mate, n >= 0)]
    pairs += [(n, far, inside & (n >= 3)), (n, beyond, mate_inside & (n >= 3))]
    pairs += [(n + 1, s, n < N - 1), (n - 1, s, n > 0)]
    pairs += [(n + 2, s, (n > 0) & (n < N - 2)), (n - 2, s, n > 2)]
    pairs += [(n + 3, s, n == 0), (n - 3, s, n == 3)]
    barrier = pltpu.get_barrier_semaphore()
    count = 0
    for i, j, cond in pairs:
        @pl.when(cond)
        def _():
            pl.semaphore_signal(barrier, inc=1, device_id=(i, j), device_id_type=MESH)
        count = count + jnp.where(cond, 1, 0)

    inner = pl.ds(PAD, NY)

    def load(i):
        return pltpu.make_async_copy(x_ref.at[0, :, i + p * (W - 1 - 2 * i)], ev.at[D + i, :, inner], load_sem.at[i])

    keep_start = pltpu.make_async_copy(x_ref.at[0], out_ref.at[0], load_sem.at[W])

    @pl.when(works)
    def _():
        for i in range(W):
            load(i).start()

    @pl.when(n == 0)
    def _():
        keep_start.start()

    zero = jnp.zeros((PAD, NZ), jnp.float32)

    def clear(i, _):
        for c in range(3):
            for top in (0, PAD + NY):
                ev[i, c, pl.ds(top, PAD), :] = zero
                od[i, c, pl.ds(top, PAD), :] = zero
        return 0

    def clear_layer(i, _):
        for c in range(3):
            for row in range(PAD, PAD + NY, 8):
                ev[i * Q + D - 1, c, pl.ds(row, 8), :] = zero
                od[i * Q + D - 1, c, pl.ds(row, 8), :] = zero
        return 0

    def clear_start(i, _):
        for c in range(3):
            for row in range(PAD, PAD + NY, 8):
                ev[i, c, pl.ds(row, 8), :] = zero
        return 0

    def clear_coarse(i, _):
        for c in range(3):
            for top in (0, PAD + CY):
                ca[i, c, pl.ds(top, PAD), :] = zero
                cb[i, c, pl.ds(top, PAD), :] = zero
        return 0

    lax.fori_loop(0, END * Q, clear, 0)
    lax.fori_loop(0, jnp.where(wall, END, 0), clear_layer, 0)
    lax.fori_loop(0, jnp.where(wall, D, 0), clear_start, 0)
    lax.fori_loop(0, 5 * CW, clear_coarse, 0)

    @pl.when(works)
    def _():
        for i in range(W):
            load(i).wait()

    pl.semaphore_wait(barrier, count)

    def remote(src, dst, send_sem, recv_sem, target):
        return pltpu.make_async_remote_copy(
            src_ref=src, dst_ref=dst, send_sem=send_sem, recv_sem=recv_sem, device_id=target, device_id_type=MESH)

    def halo(r, d):
        at = r * W * Q
        return remote(ev.at[at + D + d, :, inner], ev.at[at + D - 1 - d, :, inner], halo_s.at[r, d], halo_r.at[r, d],
                      (n, wrap(near)))

    def to_mate(r, i):
        at = r * W * Q
        return remote(ev.at[at + D + i, :, inner], ev.at[at + Q - 1 - i, :, inner], part_s.at[r, i], part_r.at[r, i],
                      (n, wrap(mate)))

    def mid_to_mate(r, i):
        at = (r * W + CW) * Q
        return remote(ev.at[at + D + i, :, inner], ev.at[at + Q - 1 - i, :, inner], mid_s.at[r, i], mid_r.at[r, i],
                      (n, wrap(mate)))

    def send_halo(r, d):
        @pl.when(inside)
        def _():
            halo(r, d).start()

    def to_next(i):
        return remote(ev.at[END * Q + D + i, :, inner], rc_end.at[i], end_s.at[i], end_r.at[i], (column(n + 1), s))

    even = lax.broadcasted_iota(jnp.int32, (CY, NZ), 1) % 2 == 0
    crow = pl.ds(PAD, CY)

    def restricted(at, c):
        def read(l, r):
            return ev[at + l, c, pl.ds(PAD + r, CY, stride=2), :]
        total = (read(0, 0) + read(0, 1)) + (read(1, 0) + read(1, 1))
        other = jnp.where(even, pltpu.roll(total, NZ - 1, 1), pltpu.roll(total, 1, 1))
        return (total + other) * 0.125

    def packed(a, b):
        return jnp.where(even, a, b)

    def unpacked(v):
        return jnp.where(even, v, pltpu.roll(v, 1, 1)), jnp.where(even, pltpu.roll(v, NZ - 1, 1), v)

    near_keep = jnp.where(wall, jnp.zeros((8, NZ), jnp.float32), 1.0)
    beyond_keep = jnp.where(mate_wall, jnp.zeros((8, NZ), jnp.float32), 1.0)

    def coarse(src, dst, lo, hi):
        items = [(c, c, near_keep if c < 2 * CW else beyond_keep if c >= 4 * CW else None) for c in range(lo, hi)]
        step(src, dst, items, (PAD, PAD + CY), coarse_rate, coarse_advect, 2, turn)

    def fine(at, l, qs):
        e, o = ev.at[pl.ds(at, W * Q + 2 * D)], od.at[pl.ds(at, (W - 1) * Q + 2 * D)]
        src, dst = (e, o) if l % 2 else (o, e)
        step(src, dst, [((l - 1) // 2 * Q + q, l // 2 * Q + q, None) for q in qs], (PAD, PAD + NY), fine_rate, fine_advect, 1, turn)

    send_old = remote(pk_old, rc_old, old_s, old_r, (column(n + 1), s))

    def one_round(r, _):
        base = r * W
        for m in range(W):
            i = W - 1 - m
            if m == 0:
                @pl.when(r == 0)
                def _():
                    to_mate(r, i).wait_recv()
                    send_halo(r, W)
            else:
                to_mate(r, i).wait_recv()
                send_halo(r, W + m)
        for l in range(1, W):
            def pair(h, _):
                fine(base * Q + 2 * h, l, [D + l, D + l + 1])
                return 0
            lax.fori_loop(0, W - l, pair, 0)

        @pl.when(r == ROUNDS - 1)
        def _():
            def restrict_layer(c, _):
                for k in range(3):
                    ca[c, k, crow, :] = restricted(2 * c, k)
                return 0
            lax.fori_loop(CW, 4 * CW, restrict_layer, 0)
            coarse(ca, cb, 2 * CW - 1, 3 * CW + 1)
            coarse(cb, cc, 2 * CW, 3 * CW)
            for k in range(3):
                pk_old[k] = packed(cc[2 * CW, k, crow, :], cc[2 * CW + 1, k, crow, :])
            send_old.start()

        def wave(k, levels):
            fixed = isinstance(k, int)
            at, first = (base * Q, D - 1 - k) if fixed else (base * Q + D - 1 - k, 0)

            @pl.when(inside)
            def _():
                for l in levels:
                    fine(at, l, [first + l])

            @pl.when(wall)
            def _():
                for l in levels:
                    if not fixed:
                        @pl.when(l > k)
                        def _():
                            fine(at, l, [first + l])
                    elif l > k:
                        fine(at, l, [first + l])

        def await_halo(k):
            @pl.when(inside)
            def _():
                halo(r, k).wait_recv()

        for k in range(W + 1):
            await_halo(k)
            wave(k, range(1, W + 1))
            if k < W:
                mid_to_mate(r, W - 1 - k).start()
            if k >= 1:
                mid_to_mate(r, W - k).wait_recv()
                for l in range(W + 1, W + k):
                    fine(base * Q, l, [Q - 1 + k - l])
                wave(k, range(W + 1, W + 1 + k))

        def sent(k):
            i = D - 1 - k

            @pl.when(r < ROUNDS - 1)
            def _():
                to_mate(r + 1, i).start()
                if k == W:
                    send_halo(r + 1, i)
                elif k == W + 1:
                    send_halo(r + 1, i)
                    to_mate(r + 1, W - 1).wait_recv()
                    send_halo(r + 1, W)
                elif k == D - 1:
                    send_halo(r + 1, 0)
                    send_halo(r + 1, 1)

            @pl.when(r == ROUNDS - 1)
            def _():
                if k == W:
                    to_next(i).start()
                elif i > 0:
                    pl.when(n > 0)(lambda: to_next(i).start())

        sent(W)

        def late(k, _):
            await_halo(k)
            wave(k, range(1, D + 1))
            for j in range(W + 1, D):
                @pl.when(k == j)
                def _():
                    sent(j)
            return 0

        lax.fori_loop(W + 1, D, late, 0)
        return 0

    def own_copy(target):
        return remote(pk_cs, rc_own, own_s, own_r, (column(target), s))

    adv_copy = remote(pk_adv, rc_adv, adv_s, adv_r, (column(n + N - 1), s))

    def r_copy(target):
        return remote(pk_r, rc_r, r_s, r_r, (column(target), s))

    def r1_copy(target):
        return remote(pk_r, rc_r1, r1_s, r1_r, (column(target), s))

    @pl.when(works)
    def _():
        for i in range(W):
            send_halo(0, i)
            to_mate(0, W - 1 - i).start()
        lax.fori_loop(0, ROUNDS, one_round, 0)
        for k in range(3):
            change = [restricted(END * Q + D + 2 * j, k) - cc[2 * CW + j, k, crow, :] for j in range(CW)]
            pk_r[k] = packed(*change)
            pk_cs[k] = packed(*(cc[2 * CW + j, k, crow, :] + change[j] for j in range(CW)))

        @pl.when(n == 0)
        def _():
            own_copy(3).start()

        @pl.when((n >= 1) & (n <= N - 3))
        def _():
            r_copy(n + 2).start()
        if N > 4:
            @pl.when((n >= 1) & (n <= N - 4))
            def _():
                r1_copy(n + 1).start()
        for i in range(W - 2, 0, -1):
            pl.when(n == 0)(lambda: to_next(i).start())
        to_next(0).start()

    def exchange(src, dst, send, recv, k):
        target, slot = [(near, 0), (mate, 1), (far, 3), (beyond, 2)][k]
        return remote(src, dst.at[slot], send.at[slot], recv.at[slot], (n, wrap(target)))

    exists = [inside, None, inside, mate_inside]

    def guarded(cond, do):
        if cond is None:
            do()
        else:
            pl.when(cond)(do)

    places = [(2 * CW - 1, -1), (4 * CW - 1, -1), (0, 1), (4 * CW, 1)]
    slot_exists = [inside, None, inside, mate_inside]

    def unpack_into(dst, slot, src):
        first, by = places[slot]

        def fill():
            for k in range(3):
                for j, v in enumerate(unpacked(src[k])):
                    dst[first + by * j, k, crow, :] = v

        def blank():
            for k in range(3):
                for j in range(CW):
                    dst[first + by * j, k, crow, :] = jnp.zeros((CY, NZ), jnp.float32)

        guarded(slot_exists[slot], fill)
        if slot_exists[slot] is not None:
            pl.when(jnp.logical_not(slot_exists[slot]))(blank)

    @pl.when(n == 1)
    def _():
        old_copy = remote(pk_old, rc_old, old_s, old_r, (column(n + 1), s))
        old_copy.wait_recv()
        for k in range(3):
            for j, v in enumerate(unpacked(rc_old[k])):
                cc[2 * CW + j, k, crow, :] = v

    @pl.when(n == 2)
    def _():
        adv_copy.wait_recv()
        for k in range(3):
            for j, v in enumerate(unpacked(rc_adv[k])):
                cc[2 * CW + j, k, crow, :] = v

    @pl.when(n >= 3)
    def _():
        r_copy(n + 2).wait_recv()
        for k in range(2):
            guarded(exists[k], lambda: exchange(rc_r, rc_rz, rz_s, rz_r, k).start())
        own_copy(n + 2).wait_recv()
        for k in range(2):
            guarded(exists[k], lambda: exchange(rc_own, rc_z, z_s, z_r, k).start())
        for k in range(3):
            for j, v in enumerate(unpacked(rc_own[k])):
                ca[2 * CW + j, k, crow, :] = v
        for k in range(2, 4):
            guarded(exists[k], lambda: exchange(rc_own, rc_z, z_s, z_r, k).start())

        def arrived(k, slot):
            guarded(slot_exists[slot], lambda: exchange(rc_own, rc_z, z_s, z_r, k).wait_recv())
            unpack_into(ca, slot, rc_z.at[slot])

        arrived(1, 1)
        arrived(0, 0)
        coarse(ca, cb, 2 * CW - 1, 3 * CW + 1)
        coarse(cb, cc, 2 * CW, 3 * CW)

        @pl.when(n == 3)
        def _():
            for k in range(3):
                pk_adv[k] = packed(cc[2 * CW, k, crow, :], cc[2 * CW + 1, k, crow, :])
            adv_copy.start()
        arrived(2, 3)
        arrived(3, 2)
        for lo, hi in ((1, 2 * CW - 1), (3 * CW + 1, 5 * CW - 1)):
            coarse(ca, cb, lo, hi)
        for lo, hi in ((CW, 2 * CW), (3 * CW, 4 * CW)):
            coarse(cb, cc, lo, hi)
        for slot in (1, 0):
            guarded(slot_exists[slot], lambda: exchange(rc_r, rc_rz, rz_s, rz_r, slot).wait_recv())
            unpack_into(ca, slot, rc_rz.at[slot])
        for k in range(3):
            for j, v in enumerate(unpacked(rc_r[k])):
                ca[2 * CW + j, k, crow, :] = v

        def add(c, _):
            for k in range(3):
                ca[c, k, crow, :] = ca[c, k, crow, :] + cc[c, k, crow, :]
            return 0

        lax.fori_loop(CW, 4 * CW, add, 0)
        coarse(ca, cb, 2 * CW - 1, 3 * CW + 1)
        coarse(cb, cc, 2 * CW, 3 * CW)

    if N > 4:
        @pl.when((n >= 2) & (n <= N - 3))
        def _():
            r1_copy(n + 1).wait_recv()
            for k in range(3):
                change = unpacked(rc_r1[k])
                pk_cs[k] = packed(*(cc[2 * CW + j, k, crow, :] + change[j] for j in range(CW)))
            own_copy(n + 2).start()

    @pl.when(n == 0)
    def _():
        keep_start.wait()

    @pl.when(n > 0)
    def _():
        @pl.when(n > 1)
        def _():
            send_old.wait_recv()
        for k in range(3):
            old = unpacked(rc_old[k])
            for j in range(CW):
                rise = cc[2 * CW + j, k, crow, :] - old[j]
                for r in range(2):
                    spread[j, k, pl.ds(r, CY, stride=2), :] = rise
        for i in range(W - 1, -1, -1):
            to_next(i).wait_recv()
            for k in range(3):
                out_ref[0, k, i + p * (W - 1 - 2 * i)] = spread[i // 2, k, pl.ds(0, NY), :] + rc_end[i, k]

    @pl.when(works)
    def _():
        send_old.wait_send()
        for i in range(W):
            to_next(i).wait_send()
            for r in range(ROUNDS):
                to_mate(r, i).wait_send()
                mid_to_mate(r, i).wait_send()

        @pl.when(inside)
        def _():
            for r in range(ROUNDS):
                for d in range(D):
                    halo(r, d).wait_send()

        @pl.when(n == 0)
        def _():
            own_copy(3).wait_send()

        @pl.when((n >= 1) & (n <= N - 3))
        def _():
            r_copy(n + 2).wait_send()
        if N > 4:
            @pl.when((n >= 1) & (n <= N - 4))
            def _():
                r1_copy(n + 1).wait_send()

            @pl.when((n >= 2) & (n <= N - 3))
            def _():
                own_copy(n + 2).wait_send()

    @pl.when(n >= 3)
    def _():
        for k in range(4):
            guarded(exists[k], lambda: exchange(rc_own, rc_z, z_s, z_r, k).wait_send())
        for k in range(2):
            guarded(exists[k], lambda: exchange(rc_r, rc_rz, rz_s, rz_r, k).wait_send())

        @pl.when(n == 3)
        def _():
            adv_copy.wait_send()


def shards(S, N, starts):
    W, NY, NZ = starts.shape[2:]
    D, Q = 2 * W, 4 * W
    assert W == 4 and FSTEPS % D == 0 and CSTEPS == 2 and S % 2 == 0 and N > 3
    f32 = jnp.float32
    CW, CY, ROUNDS, END = W // 2, NY // 2, FSTEPS // D, FSTEPS // 2
    pack = (3, CY, NZ)
    coarse = pltpu.VMEM((5 * CW, 3, CY + 2 * PAD, NZ), f32)
    dma = pltpu.SemaphoreType.DMA
    return pl.pallas_call(
        functools.partial(kernel, S, N),
        out_shape=jax.ShapeDtypeStruct(starts.shape, f32),
        in_specs=[pl.BlockSpec(memory_space=pltpu.HBM)],
        out_specs=pl.BlockSpec(memory_space=pltpu.VMEM),
        scratch_shapes=[
            pltpu.VMEM(((END + 1) * Q + D, 3, NY + 2 * PAD, NZ), f32),
            pltpu.VMEM((END * Q + D, 3, NY + 2 * PAD, NZ), f32),
            coarse, coarse, coarse,
            pltpu.VMEM(pack, f32), pltpu.VMEM(pack, f32), pltpu.VMEM(pack, f32), pltpu.VMEM(pack, f32),
            pltpu.VMEM(pack, f32), pltpu.VMEM(pack, f32), pltpu.VMEM((4,) + pack, f32),
            pltpu.VMEM(pack, f32), pltpu.VMEM((2,) + pack, f32), pltpu.VMEM(pack, f32), pltpu.VMEM(pack, f32),
            pltpu.VMEM((W, 3, NY, NZ), f32),
            pltpu.VMEM((CW, 3, NY + PAD, NZ), f32),
            dma((W + 1,)),
            dma((ROUNDS, D)), dma((ROUNDS, D)), dma((ROUNDS, W)), dma((ROUNDS, W)), dma((ROUNDS, W)), dma((ROUNDS, W)),
            dma((W,)), dma((W,)), dma, dma, dma, dma, dma((4,)), dma((4,)), dma, dma, dma((2,)), dma((2,)), dma, dma, dma, dma,
        ],
        compiler_params=pltpu.CompilerParams(collective_id=0, has_side_effects=True, vmem_limit_bytes=48 * 2**20),
    )(pltpu.with_memory_space_constraint(starts, pltpu.HBM))


def solution(mesh):
    placed = P("cuts", None, "space", None, None)
    return jax.shard_map(
        functools.partial(shards, mesh.shape["space"], mesh.shape["cuts"]),
        mesh=mesh, in_specs=(placed,), out_specs=placed, check_vma=False)
```

```python
import functools

import jax
import jax.numpy as jnp
from jax import lax
from jax.experimental import pallas as pl
from jax.experimental.pallas import tpu as pltpu
from jax.sharding import PartitionSpec as P

FSTEPS = 16
CSTEPS = 2

fine_rate = 0.08
fine_advect = 0.04
coarse_rate = 0.16
coarse_advect = 0.16

PAD = 8
MESH = pl.DeviceIdType.MESH


def step(src, dst, items, rows, rate, advect, shift, turn):
    lanes = src.shape[-1]
    lane = lax.broadcasted_iota(jnp.int32, (8, lanes), 1)
    first, last = lane < shift, lane >= lanes - shift
    rzp, azp = jnp.where(last, 0.0, rate), jnp.where(last, 0.0, advect)
    rzm, azm = jnp.where(first, 0.0, rate), jnp.where(first, 0.0, advect)
    for row in range(rows[0], rows[1], 8):
        for si, di, keep in items:
            v = [src[si, c, pl.ds(row, 8), :] for c in range(3)]
            ax, ay = (advect * turn) * v[0], advect * v[1]
            xp, xm, yp, ym = rate - ax, rate + ax, rate - ay, rate + ay
            zp, zm = rzp - azp * v[2], rzm + azm * v[2]
            for c in range(3):
                x_part = xp * src[si + 1, c, pl.ds(row, 8), :] + xm * src[si - 1, c, pl.ds(row, 8), :]
                y_part = yp * src[si, c, pl.ds(row + 1, 8), :] + ym * src[si, c, pl.ds(row - 1, 8), :]
                z_part = zp * pltpu.roll(v[c], lanes - shift, 1) + zm * pltpu.roll(v[c], shift, 1)
                value = ((1.0 - 6.0 * rate) * v[c] + x_part) + (y_part + z_part)
                dst[di, c, pl.ds(row, 8), :] = value if keep is None else value * keep


def kernel(S, N, x_ref, out_ref, ev, od, ca, cb, cc, pk_old, pk_r, pk_cs, pk_adv, rc_old, rc_own, rc_z, rc_r, rc_rz, rc_r1,
           rc_adv, rc_end, spread, load_sem, halo_s, halo_r, part_s, part_r, mid_s, mid_r, end_s, end_r, old_s, old_r,
           own_s, own_r, z_s, z_r, r_s, r_r, rz_s, rz_r, r1_s, r1_r,
           adv_s, adv_r):
    n, s = lax.axis_index("cuts"), lax.axis_index("space")
    W, NY, NZ = x_ref.shape[2], x_ref.shape[3], x_ref.shape[4]
    CW, CY, Q, D = W // 2, NY // 2, 4 * W, 2 * W
    ROUNDS = FSTEPS // D
    END = FSTEPS // 2
    p = lax.rem(s, 2)
    way = 1 - 2 * p
    turn = way.astype(jnp.float32)
    near, mate = s - way, s + way
    far, beyond = s - 2 * way, s + 2 * way
    wall = (near < 0) | (near >= S)
    mate_wall = (beyond < 0) | (beyond >= S)
    inside = jnp.logical_not(wall)
    mate_inside = jnp.logical_not(mate_wall)
    works = n < N - 1

    def wrap(i):
        return lax.rem(i + 2 * S, S)

    def column(i):
        return lax.rem(i, N)

    pairs = [(n, near, inside), (n, mate, n >= 0)]
    pairs += [(n, far, inside & (n >= 3)), (n, beyond, mate_inside & (n >= 3))]
    pairs += [(n + 1, s, n < N - 1), (n - 1, s, n > 0)]
    pairs += [(n + 2, s, (n > 0) & (n < N - 2)), (n - 2, s, n > 2)]
    pairs += [(n + 3, s, n == 0), (n - 3, s, n == 3)]
    barrier = pltpu.get_barrier_semaphore()
    count = 0
    for i, j, cond in pairs:
        @pl.when(cond)
        def _():
            pl.semaphore_signal(barrier, inc=1, device_id=(i, j), device_id_type=MESH)
        count = count + jnp.where(cond, 1, 0)

    inner = pl.ds(PAD, NY)

    def load(i):
        return pltpu.make_async_copy(x_ref.at[0, :, i + p * (W - 1 - 2 * i)], ev.at[D + i, :, inner], load_sem.at[i])

    keep_start = pltpu.make_async_copy(x_ref.at[0], out_ref.at[0], load_sem.at[W])

    @pl.when(works)
    def _():
        for i in range(W):
            load(i).start()

    @pl.when(n == 0)
    def _():
        keep_start.start()

    zero = jnp.zeros((PAD, NZ), jnp.float32)

    def clear(i, _):
        for c in range(3):
            for top in (0, PAD + NY):
                ev[i, c, pl.ds(top, PAD), :] = zero
                od[i, c, pl.ds(top, PAD), :] = zero
        return 0

    def clear_layer(i, _):
        for c in range(3):
            for row in range(PAD, PAD + NY, 8):
                ev[i * Q + D - 1, c, pl.ds(row, 8), :] = zero
                od[i * Q + D - 1, c, pl.ds(row, 8), :] = zero
        return 0

    def clear_start(i, _):
        for c in range(3):
            for row in range(PAD, PAD + NY, 8):
                ev[i, c, pl.ds(row, 8), :] = zero
        return 0

    def clear_coarse(i, _):
        for c in range(3):
            for top in (0, PAD + CY):
                ca[i, c, pl.ds(top, PAD), :] = zero
                cb[i, c, pl.ds(top, PAD), :] = zero
        return 0

    lax.fori_loop(0, END * Q, clear, 0)
    lax.fori_loop(0, jnp.where(wall, END, 0), clear_layer, 0)
    lax.fori_loop(0, jnp.where(wall, D, 0), clear_start, 0)
    lax.fori_loop(0, 5 * CW, clear_coarse, 0)

    @pl.when(works)
    def _():
        for i in range(W):
            load(i).wait()

    pl.semaphore_wait(barrier, count)

    def remote(src, dst, send_sem, recv_sem, target):
        return pltpu.make_async_remote_copy(
            src_ref=src, dst_ref=dst, send_sem=send_sem, recv_sem=recv_sem, device_id=target, device_id_type=MESH)

    def halo(r, d):
        at = r * W * Q
        return remote(ev.at[at + D + d, :, inner], ev.at[at + D - 1 - d, :, inner], halo_s.at[r, d], halo_r.at[r, d],
                      (n, wrap(near)))

    def to_mate(r, i):
        at = r * W * Q
        return remote(ev.at[at + D + i, :, inner], ev.at[at + Q - 1 - i, :, inner], part_s.at[r, i], part_r.at[r, i],
                      (n, wrap(mate)))

    def mid_to_mate(r, i):
        at = (r * W + CW) * Q
        return remote(ev.at[at + D + i, :, inner], ev.at[at + Q - 1 - i, :, inner], mid_s.at[r, i], mid_r.at[r, i],
                      (n, wrap(mate)))

    def send_halo(r, d):
        @pl.when(inside)
        def _():
            halo(r, d).start()

    def to_next(i):
        return remote(ev.at[END * Q + D + i, :, inner], rc_end.at[i], end_s.at[i], end_r.at[i], (column(n + 1), s))

    even = lax.broadcasted_iota(jnp.int32, (CY, NZ), 1) % 2 == 0
    crow = pl.ds(PAD, CY)

    def restricted(at, c):
        def read(l, r):
            return ev[at + l, c, pl.ds(PAD + r, CY, stride=2), :]
        total = (read(0, 0) + read(0, 1)) + (read(1, 0) + read(1, 1))
        other = jnp.where(even, pltpu.roll(total, NZ - 1, 1), pltpu.roll(total, 1, 1))
        return (total + other) * 0.125

    def packed(a, b):
        return jnp.where(even, a, b)

    def unpacked(v):
        return jnp.where(even, v, pltpu.roll(v, 1, 1)), jnp.where(even, pltpu.roll(v, NZ - 1, 1), v)

    near_keep = jnp.where(wall, jnp.zeros((8, NZ), jnp.float32), 1.0)
    beyond_keep = jnp.where(mate_wall, jnp.zeros((8, NZ), jnp.float32), 1.0)

    def coarse(src, dst, lo, hi):
        items = [(c, c, near_keep if c < 2 * CW else beyond_keep if c >= 4 * CW else None) for c in range(lo, hi)]
        step(src, dst, items, (PAD, PAD + CY), coarse_rate, coarse_advect, 2, turn)

    def fine(at, l, qs):
        e, o = ev.at[pl.ds(at, W * Q + 2 * D)], od.at[pl.ds(at, (W - 1) * Q + 2 * D)]
        src, dst = (e, o) if l % 2 else (o, e)
        step(src, dst, [((l - 1) // 2 * Q + q, l // 2 * Q + q, None) for q in qs], (PAD, PAD + NY), fine_rate, fine_advect, 1, turn)

    send_old = remote(pk_old, rc_old, old_s, old_r, (column(n + 1), s))

    def one_round(r, _):
        base = r * W
        for m in range(W):
            i = W - 1 - m
            if m == 0:
                @pl.when(r == 0)
                def _():
                    to_mate(r, i).wait_recv()
                    send_halo(r, W)
            else:
                to_mate(r, i).wait_recv()
                send_halo(r, W + m)
        for l in range(1, W):
            def pair(h, _):
                fine(base * Q + 2 * h, l, [D + l, D + l + 1])
                return 0
            lax.fori_loop(0, W - l, pair, 0)

        @pl.when(r == ROUNDS - 1)
        def _():
            def restrict_layer(c, _):
                for k in range(3):
                    ca[c, k, crow, :] = restricted(2 * c, k)
                return 0
            lax.fori_loop(CW, 4 * CW, restrict_layer, 0)
            coarse(ca, cb, 2 * CW - 1, 3 * CW + 1)
            coarse(cb, cc, 2 * CW, 3 * CW)
            for k in range(3):
                pk_old[k] = packed(cc[2 * CW, k, crow, :], cc[2 * CW + 1, k, crow, :])
            send_old.start()

        def wave(k, levels):
            fixed = isinstance(k, int)
            at, first = (base * Q, D - 1 - k) if fixed else (base * Q + D - 1 - k, 0)

            @pl.when(inside)
            def _():
                for l in levels:
                    fine(at, l, [first + l])

            @pl.when(wall)
            def _():
                for l in levels:
                    if not fixed:
                        @pl.when(l > k)
                        def _():
                            fine(at, l, [first + l])
                    elif l > k:
                        fine(at, l, [first + l])

        def await_halo(k):
            @pl.when(inside)
            def _():
                halo(r, k).wait_recv()

        for k in range(W + 1):
            await_halo(k)
            wave(k, range(1, W + 1))
            if k < W:
                mid_to_mate(r, W - 1 - k).start()
            if k >= 1:
                mid_to_mate(r, W - k).wait_recv()
                for l in range(W + 1, W + k):
                    fine(base * Q, l, [Q - 1 + k - l])
                wave(k, range(W + 1, W + 1 + k))

        def sent(k):
            i = D - 1 - k

            @pl.when(r < ROUNDS - 1)
            def _():
                if k == D - 1:
                    send_halo(r + 1, 0)
                to_mate(r + 1, i).start()
                if k == W:
                    send_halo(r + 1, i)
                elif k == W + 1:
                    send_halo(r + 1, i)
                    to_mate(r + 1, W - 1).wait_recv()
                    send_halo(r + 1, W)
                elif k == D - 1:
                    send_halo(r + 1, 1)

            @pl.when(r == ROUNDS - 1)
            def _():
                if k == W:
                    to_next(i).start()
                elif i > 0:
                    pl.when(n > 0)(lambda: to_next(i).start())

        sent(W)

        def late(k, _):
            await_halo(k)
            wave(k, range(1, D + 1))
            for j in range(W + 1, D):
                @pl.when(k == j)
                def _():
                    sent(j)
            return 0

        lax.fori_loop(W + 1, D, late, 0)
        return 0

    def own_copy(target):
        return remote(pk_cs, rc_own, own_s, own_r, (column(target), s))

    adv_copy = remote(pk_adv, rc_adv, adv_s, adv_r, (column(n + N - 1), s))

    def r_copy(target):
        return remote(pk_r, rc_r, r_s, r_r, (column(target), s))

    def r1_copy(target):
        return remote(pk_r, rc_r1, r1_s, r1_r, (column(target), s))

    @pl.when(works)
    def _():
        for i in range(W):
            send_halo(0, i)
            to_mate(0, W - 1 - i).start()
        lax.fori_loop(0, ROUNDS, one_round, 0)
        for k in range(3):
            change = [restricted(END * Q + D + 2 * j, k) - cc[2 * CW + j, k, crow, :] for j in range(CW)]
            pk_r[k] = packed(*change)
            pk_cs[k] = packed(*(cc[2 * CW + j, k, crow, :] + change[j] for j in range(CW)))

        @pl.when(n == 0)
        def _():
            own_copy(3).start()

        @pl.when((n >= 1) & (n <= N - 3))
        def _():
            r_copy(n + 2).start()
        if N > 4:
            @pl.when((n >= 1) & (n <= N - 4))
            def _():
                r1_copy(n + 1).start()
        for i in range(W - 2, 0, -1):
            pl.when(n == 0)(lambda: to_next(i).start())
        to_next(0).start()

    def exchange(src, dst, send, recv, k):
        target, slot = [(near, 0), (mate, 1), (far, 3), (beyond, 2)][k]
        return remote(src, dst.at[slot], send.at[slot], recv.at[slot], (n, wrap(target)))

    exists = [inside, None, inside, mate_inside]

    def guarded(cond, do):
        if cond is None:
            do()
        else:
            pl.when(cond)(do)

    places = [(2 * CW - 1, -1), (4 * CW - 1, -1), (0, 1), (4 * CW, 1)]
    slot_exists = [inside, None, inside, mate_inside]

    def unpack_into(dst, slot, src):
        first, by = places[slot]

        def fill():
            for k in range(3):
                for j, v in enumerate(unpacked(src[k])):
                    dst[first + by * j, k, crow, :] = v

        def blank():
            for k in range(3):
                for j in range(CW):
                    dst[first + by * j, k, crow, :] = jnp.zeros((CY, NZ), jnp.float32)

        guarded(slot_exists[slot], fill)
        if slot_exists[slot] is not None:
            pl.when(jnp.logical_not(slot_exists[slot]))(blank)

    @pl.when(n == 1)
    def _():
        old_copy = remote(pk_old, rc_old, old_s, old_r, (column(n + 1), s))
        old_copy.wait_recv()
        for k in range(3):
            for j, v in enumerate(unpacked(rc_old[k])):
                cc[2 * CW + j, k, crow, :] = v

    @pl.when(n == 2)
    def _():
        adv_copy.wait_recv()
        for k in range(3):
            for j, v in enumerate(unpacked(rc_adv[k])):
                cc[2 * CW + j, k, crow, :] = v

    @pl.when(n >= 3)
    def _():
        r_copy(n + 2).wait_recv()
        for k in range(2):
            guarded(exists[k], lambda: exchange(rc_r, rc_rz, rz_s, rz_r, k).start())
        own_copy(n + 2).wait_recv()
        for k in range(2):
            guarded(exists[k], lambda: exchange(rc_own, rc_z, z_s, z_r, k).start())
        for k in range(3):
            for j, v in enumerate(unpacked(rc_own[k])):
                ca[2 * CW + j, k, crow, :] = v
        for k in range(2, 4):
            guarded(exists[k], lambda: exchange(rc_own, rc_z, z_s, z_r, k).start())

        def arrived(k, slot):
            guarded(slot_exists[slot], lambda: exchange(rc_own, rc_z, z_s, z_r, k).wait_recv())
            unpack_into(ca, slot, rc_z.at[slot])

        arrived(1, 1)
        arrived(0, 0)
        coarse(ca, cb, 2 * CW - 1, 3 * CW + 1)
        coarse(cb, cc, 2 * CW, 3 * CW)

        @pl.when(n == 3)
        def _():
            for k in range(3):
                pk_adv[k] = packed(cc[2 * CW, k, crow, :], cc[2 * CW + 1, k, crow, :])
            adv_copy.start()
        arrived(2, 3)
        arrived(3, 2)
        for lo, hi in ((1, 2 * CW - 1), (3 * CW + 1, 5 * CW - 1)):
            coarse(ca, cb, lo, hi)
        for lo, hi in ((CW, 2 * CW), (3 * CW, 4 * CW)):
            coarse(cb, cc, lo, hi)
        for slot in (1, 0):
            guarded(slot_exists[slot], lambda: exchange(rc_r, rc_rz, rz_s, rz_r, slot).wait_recv())
            unpack_into(ca, slot, rc_rz.at[slot])
        for k in range(3):
            for j, v in enumerate(unpacked(rc_r[k])):
                ca[2 * CW + j, k, crow, :] = v

        def add(c, _):
            for k in range(3):
                ca[c, k, crow, :] = ca[c, k, crow, :] + cc[c, k, crow, :]
            return 0

        lax.fori_loop(CW, 4 * CW, add, 0)
        coarse(ca, cb, 2 * CW - 1, 3 * CW + 1)
        coarse(cb, cc, 2 * CW, 3 * CW)

    if N > 4:
        @pl.when((n >= 2) & (n <= N - 3))
        def _():
            r1_copy(n + 1).wait_recv()
            for k in range(3):
                change = unpacked(rc_r1[k])
                pk_cs[k] = packed(*(cc[2 * CW + j, k, crow, :] + change[j] for j in range(CW)))
            own_copy(n + 2).start()

    @pl.when(n == 0)
    def _():
        keep_start.wait()

    @pl.when(n > 0)
    def _():
        @pl.when(n > 1)
        def _():
            send_old.wait_recv()
        for k in range(3):
            old = unpacked(rc_old[k])
            for j in range(CW):
                rise = cc[2 * CW + j, k, crow, :] - old[j]
                for r in range(2):
                    spread[j, k, pl.ds(r, CY, stride=2), :] = rise
        for i in range(W - 1, -1, -1):
            to_next(i).wait_recv()
            for k in range(3):
                out_ref[0, k, i + p * (W - 1 - 2 * i)] = spread[i // 2, k, pl.ds(0, NY), :] + rc_end[i, k]

    @pl.when(works)
    def _():
        send_old.wait_send()
        for i in range(W):
            to_next(i).wait_send()
            for r in range(ROUNDS):
                to_mate(r, i).wait_send()
                mid_to_mate(r, i).wait_send()

        @pl.when(inside)
        def _():
            for r in range(ROUNDS):
                for d in range(D):
                    halo(r, d).wait_send()

        @pl.when(n == 0)
        def _():
            own_copy(3).wait_send()

        @pl.when((n >= 1) & (n <= N - 3))
        def _():
            r_copy(n + 2).wait_send()
        if N > 4:
            @pl.when((n >= 1) & (n <= N - 4))
            def _():
                r1_copy(n + 1).wait_send()

            @pl.when((n >= 2) & (n <= N - 3))
            def _():
                own_copy(n + 2).wait_send()

    @pl.when(n >= 3)
    def _():
        for k in range(4):
            guarded(exists[k], lambda: exchange(rc_own, rc_z, z_s, z_r, k).wait_send())
        for k in range(2):
            guarded(exists[k], lambda: exchange(rc_r, rc_rz, rz_s, rz_r, k).wait_send())

        @pl.when(n == 3)
        def _():
            adv_copy.wait_send()


def shards(S, N, starts):
    W, NY, NZ = starts.shape[2:]
    D, Q = 2 * W, 4 * W
    assert W == 4 and FSTEPS % D == 0 and CSTEPS == 2 and S % 2 == 0 and N > 3
    f32 = jnp.float32
    CW, CY, ROUNDS, END = W // 2, NY // 2, FSTEPS // D, FSTEPS // 2
    pack = (3, CY, NZ)
    coarse = pltpu.VMEM((5 * CW, 3, CY + 2 * PAD, NZ), f32)
    dma = pltpu.SemaphoreType.DMA
    return pl.pallas_call(
        functools.partial(kernel, S, N),
        out_shape=jax.ShapeDtypeStruct(starts.shape, f32),
        in_specs=[pl.BlockSpec(memory_space=pltpu.HBM)],
        out_specs=pl.BlockSpec(memory_space=pltpu.VMEM),
        scratch_shapes=[
            pltpu.VMEM(((END + 1) * Q + D, 3, NY + 2 * PAD, NZ), f32),
            pltpu.VMEM((END * Q + D, 3, NY + 2 * PAD, NZ), f32),
            coarse, coarse, coarse,
            pltpu.VMEM(pack, f32), pltpu.VMEM(pack, f32), pltpu.VMEM(pack, f32), pltpu.VMEM(pack, f32),
            pltpu.VMEM(pack, f32), pltpu.VMEM(pack, f32), pltpu.VMEM((4,) + pack, f32),
            pltpu.VMEM(pack, f32), pltpu.VMEM((2,) + pack, f32), pltpu.VMEM(pack, f32), pltpu.VMEM(pack, f32),
            pltpu.VMEM((W, 3, NY, NZ), f32),
            pltpu.VMEM((CW, 3, NY + PAD, NZ), f32),
            dma((W + 1,)),
            dma((ROUNDS, D)), dma((ROUNDS, D)), dma((ROUNDS, W)), dma((ROUNDS, W)), dma((ROUNDS, W)), dma((ROUNDS, W)),
            dma((W,)), dma((W,)), dma, dma, dma, dma, dma((4,)), dma((4,)), dma, dma, dma((2,)), dma((2,)), dma, dma, dma, dma,
        ],
        compiler_params=pltpu.CompilerParams(collective_id=0, has_side_effects=True, vmem_limit_bytes=48 * 2**20),
    )(pltpu.with_memory_space_constraint(starts, pltpu.HBM))


def solution(mesh):
    placed = P("cuts", None, "space", None, None)
    return jax.shard_map(
        functools.partial(shards, mesh.shape["space"], mesh.shape["cuts"]),
        mesh=mesh, in_specs=(placed,), out_specs=placed, check_vma=False)
```
